32 devices in a mesh: row: 4 (over y, x), col: 8 (over z, core).
Axes of the slice: x: 2, y: 2, z: 4, core: 2. Of those that a mesh axis runs over, the one named last changes fastest.
Arguments:
- view_a: bfloat16 [3072, 8192], P(('row', 'col')), may hold values from -1000 to 1000
- view_b: bfloat16 [3072, 8192], P(('row', 'col')), may hold values from -1000 to 1000
Outputs:
- correlation: float32 [8192, 8192], P('row', 'col')
- loss: float32 [], replicated
The draws below stay inside these ranges and needn't reach their ends.
All inputs are finite; a program needn't handle non-finite values.
Results may differ from the reference program's by a relative error of at most 0.0013.
Values may be sent and summed in bfloat16 or wider, within the bound.
No kernel may reach another device: no remote copies, remote signals or barrier semaphores. Data moves between devices by JAX's collectives and lax.ppermute only.
A program may use at most 192 MiB of HBM per device.

```python
import jax
import jax.numpy as jnp
from jax import lax

D = 8192
TOKENS = 3072


def draw_pair(key):
    keys = jax.random.split(jax.random.fold_in(key, 11), 6)
    ramp = jnp.arange(TOKENS, dtype=jnp.float32) / max(TOKENS - 1, 1)
    row_scale = (1.0 + 2.0 * ramp) * jnp.exp(jax.random.uniform(keys[0], (TOKENS,), jnp.float32, 0.0, jnp.log(3.0)))
    col_scale = jnp.exp(jax.random.uniform(keys[1], (D,), jnp.float32, 0.0, jnp.log(10.0)))
    mixing = jax.random.uniform(keys[2], (D,), jnp.float32, 0.2, 0.95)
    offset = 0.5 * jax.random.normal(keys[3], (D,), jnp.float32)
    base = jax.random.normal(keys[4], (TOKENS, D), jnp.float32)
    noise = jax.random.normal(keys[5], (TOKENS, D), jnp.float32)
    other = mixing * base + jnp.sqrt(1.0 - mixing * mixing) * noise
    scale = row_scale[:, None] * col_scale[None, :]
    first = jnp.clip((base + offset) * scale, -1000.0, 1000.0)
    second = jnp.clip((other + offset) * scale, -1000.0, 1000.0)
    return (first, second)


def draw_view_a(key, part):
    return draw_pair(key)[0].astype(jnp.bfloat16)


def draw_view_b(key, part):
    return draw_pair(key)[1].astype(jnp.bfloat16)


def setup_inputs(seed: int = 0) -> dict:
    seeds = jax.random.split(jax.random.key(seed), 3)
    return {
        "view_a": draw_view_a(jax.random.fold_in(seeds[2], 71), 0),
        "view_b": draw_view_b(jax.random.fold_in(seeds[2], 71), 0),
    }


def normalize(view):
    values = view.astype(jnp.float32)
    count = view.shape[0]
    mean = lax.optimization_barrier(jnp.sum(values, 0)) / count
    var = lax.optimization_barrier(jnp.sum(values * values, 0)) / count - mean * mean
    return ((values - mean) * lax.rsqrt(var + 1e-05)).astype(jnp.bfloat16)

def reference(view_a, view_b):
    norm_a = normalize(view_a).astype(jnp.float32)
    norm_b = normalize(view_b).astype(jnp.float32)
    product = lax.dot_general(norm_a, norm_b, (((0,), (0,)), ((), ())), precision=lax.Precision.HIGHEST, preferred_element_type=jnp.float32)
    correlation = product / view_a.shape[0]
    diag = jnp.diagonal(correlation)
    total = 0.0051 * jnp.sum(correlation * correlation) + jnp.sum((1.0 - diag) ** 2 - 0.0051 * diag * diag)
    loss = total / view_a.shape[1]
    return (correlation, loss)
```

```python
import jax
import jax.numpy as jnp
from jax import lax
from jax.experimental import pallas as pl
from jax.experimental.pallas import tpu as pltpu
from jax.sharding import PartitionSpec as P

CHUNKS = 1
EPS = 1e-05
WEIGHT = 0.0051


def pick(total, want):
    block = min(want, total)
    while total % block:
        block //= 2
    return block


def normalized(values, count):
    values = values.astype(jnp.float32)
    mean = jnp.sum(values, 0, keepdims=True) / count
    var = jnp.sum(values * values, 0, keepdims=True) / count - mean * mean
    return ((values - mean) * lax.rsqrt(var + EPS)).astype(jnp.bfloat16)


def norm_kernel(x_ref, o_ref, *, count):
    o_ref[...] = normalized(x_ref[...], count)


def normalize(x, count):
    block = pick(x.shape[1], 256)
    spec = pl.BlockSpec((x.shape[0], block), lambda i: (0, i))
    return pl.pallas_call(
        lambda x_ref, o_ref: norm_kernel(x_ref, o_ref, count=count),
        grid=(x.shape[1] // block,),
        in_specs=[spec],
        out_specs=spec,
        out_shape=jax.ShapeDtypeStruct(x.shape, jnp.bfloat16),
        compiler_params=pltpu.CompilerParams(vmem_limit_bytes=48 * 1024 * 1024),
        name="normalize",
    )(x)


def correlate(left, right, base, rows, first, previous, count):
    tokens, width = left.shape
    cols = right.shape[1]
    block = pick(width, 256)
    start = first // block

    def kernel(base_ref, left_ref, right_ref, *refs):
        out_ref, loss_ref = refs[-2], refs[-1]
        step = pl.program_id(0)
        left_norm = normalized(left_ref[...], count)
        product = lax.dot_general(left_norm, right_ref[...], (((0,), (0,)), ((), ())), preferred_element_type=jnp.float32)
        corr = product / count
        out_ref[...] = corr
        row_ids = base_ref[0] + step * block + lax.broadcasted_iota(jnp.int32, corr.shape, 0)
        col_ids = base_ref[1] + lax.broadcasted_iota(jnp.int32, corr.shape, 1)
        squared = corr * corr
        terms = jnp.where(row_ids == col_ids, (1.0 - corr) * (1.0 - corr), WEIGHT * squared)
        part = jnp.sum(terms.reshape(block // 8, 8, cols), 0)

        @pl.when(step == 0)
        def _():
            loss_ref[...] = part

        @pl.when(step > 0)
        def _():
            loss_ref[...] += part

    in_specs = [
        pl.BlockSpec(memory_space=pltpu.SMEM),
        pl.BlockSpec((tokens, block), lambda i: (0, i)),
        pl.BlockSpec((tokens, cols), lambda i: (0, 0)),
    ]
    args = [base, left, right]
    aliases = {}
    if previous is not None:
        in_specs.append(pl.BlockSpec(memory_space=pl.ANY))
        args.append(previous)
        aliases = {3: 0}
    return pl.pallas_call(
        kernel,
        grid=(width // block,),
        in_specs=in_specs,
        out_specs=[
            pl.BlockSpec((block, cols), lambda i: (start + i, 0)),
            pl.BlockSpec((8, cols), lambda i: (0, 0)),
        ],
        out_shape=[
            jax.ShapeDtypeStruct((rows, cols), jnp.float32),
            jax.ShapeDtypeStruct((8, cols), jnp.float32),
        ],
        input_output_aliases=aliases,
        compiler_params=pltpu.CompilerParams(vmem_limit_bytes=56 * 1024 * 1024),
        name="correlate",
    )(*args)


def swap(x, axis, k):
    if k == 0:
        return x
    return lax.ppermute(x, axis, [(i, i ^ k) for i in range(lax.axis_size(axis))])


def shards(view_a, view_b):
    tokens, width = view_a.shape
    n_row = lax.axis_size("row")
    n_col = lax.axis_size("col")
    row = lax.axis_index("row")
    col = lax.axis_index("col")
    count = tokens * n_row * n_col
    rows = width // n_row
    cols = width // n_col

    left = jnp.stack([
        swap(lax.dynamic_slice_in_dim(view_a, (row ^ k) * rows, rows, 1), "row", k) for k in range(n_row)
    ])
    right = jnp.zeros((n_col, tokens, cols), view_b.dtype)
    for k in range(n_col):
        part = swap(lax.dynamic_slice_in_dim(view_b, (col ^ k) * cols, cols, 1), "col", k)
        right = lax.dynamic_update_slice_in_dim(right, part[None], col ^ k, 0)
    right = jnp.stack([swap(right, "row", k) for k in range(n_row)], 1)
    right = normalize(right.reshape(count, cols), count)

    step = rows // CHUNKS
    gathered = [
        lax.all_gather(left[:, :, q * step:(q + 1) * step].reshape(n_row * tokens, step), "col", axis=0, tiled=True)
        for q in range(CHUNKS)
    ]
    correlation = None
    parts = []
    for q in range(CHUNKS):
        base = jnp.stack([row * rows + q * step, col * cols]).astype(jnp.int32)
        correlation, part = correlate(gathered[q], right, base, rows, q * step, correlation, count)
        parts.append(part)
    loss = jnp.sum(sum(parts).reshape(8, -1, 128), 1)
    loss = jnp.broadcast_to(jnp.sum(loss), (8, 128))
    for axis, size in (("col", n_col), ("row", n_row)):
        k = 1
        while k < size:
            loss = loss + swap(loss, axis, k)
            k *= 2
    return (correlation, loss[0, 0] / width)


def solution(mesh):
    return jax.shard_map(
        shards,
        mesh=mesh,
        in_specs=(P(("row", "col"), None), P(("row", "col"), None)),
        out_specs=(P("row", "col"), P()),
        check_vma=False,
    )
```

```python
import jax
import jax.numpy as jnp
from jax import lax
from jax.experimental import pallas as pl
from jax.experimental.pallas import tpu as pltpu
from jax.sharding import PartitionSpec as P


CHUNKS = 1
EPS = 1e-05
WEIGHT = 0.0051


def pick(total, want):
    block = min(want, total)
    while total % block:
        block //= 2
    return block


def normalized(values, count):
    values = values.astype(jnp.float32)
    mean = jnp.sum(values, 0, keepdims=True) / count
    var = jnp.sum(values * values, 0, keepdims=True) / count - mean * mean
    return ((values - mean) * lax.rsqrt(var + EPS)).astype(jnp.bfloat16)


def normalize(parts, col, count):
    n_col, tokens, cols = parts[0].shape
    n_row = len(parts)
    block = pick(cols, 256)

    def kernel(col_ref, *refs):
        out_ref = refs[-1]
        total = jnp.zeros((1, block), jnp.float32)
        squares = jnp.zeros((1, block), jnp.float32)
        for ref in refs[:-1]:
            for j in range(n_col):
                values = ref[j].astype(jnp.float32)
                total += jnp.sum(values, 0, keepdims=True)
                squares += jnp.sum(values * values, 0, keepdims=True)
        mean = total / count
        scale = lax.rsqrt(squares / count - mean * mean + EPS)
        for k, ref in enumerate(refs[:-1]):
            for j in range(n_col):
                values = ref[j].astype(jnp.float32)
                out_ref[(col_ref[0] ^ j) * n_row + k] = ((values - mean) * scale).astype(jnp.bfloat16)

    return pl.pallas_call(
        kernel,
        grid=(cols // block,),
        in_specs=[pl.BlockSpec(memory_space=pltpu.SMEM)]
        + [pl.BlockSpec((n_col, tokens, block), lambda i: (0, 0, i))] * n_row,
        out_specs=pl.BlockSpec((n_col * n_row, tokens, block), lambda i: (0, 0, i)),
        out_shape=jax.ShapeDtypeStruct((n_col * n_row, tokens, cols), jnp.bfloat16),
        compiler_params=pltpu.CompilerParams(vmem_limit_bytes=48 * 1024 * 1024),
        name="normalize",
    )(col.reshape(1).astype(jnp.int32), *parts).reshape(count, cols)


def correlate(left, right, base, rows, first, previous, count):
    tokens, width = left.shape
    cols = right.shape[1]
    block = pick(width, 256)
    start = first // block

    steps = width // block

    def kernel(base_ref, left_ref, right_ref, *refs):
        out_ref, loss_ref, norm_ref = refs[-3], refs[-2], refs[-1]
        step = pl.program_id(0) - 1

        @pl.when(step < 0)
        def _():
            norm_ref[1] = jnp.zeros((tokens, block), jnp.bfloat16)

        slot = (step + 1) % 2
        product = lax.dot_general(norm_ref[1 - slot], right_ref[...], (((0,), (0,)), ((), ())), preferred_element_type=jnp.float32)
        corr = product / count
        norm_ref[slot] = normalized(left_ref[...], count)
        out_ref[...] = corr
        row_ids = base_ref[0] + step * block + lax.broadcasted_iota(jnp.int32, corr.shape, 0)
        col_ids = base_ref[1] + lax.broadcasted_iota(jnp.int32, corr.shape, 1)
        squared = corr * corr
        terms = jnp.where(row_ids == col_ids, (1.0 - corr) * (1.0 - corr), WEIGHT * squared)
        part = jnp.sum(terms.reshape(block // 8, 8, cols), 0)

        @pl.when(step <= 0)
        def _():
            loss_ref[...] = part

        @pl.when(step > 0)
        def _():
            loss_ref[...] += part

    in_specs = [
        pl.BlockSpec(memory_space=pltpu.SMEM),
        pl.BlockSpec((tokens, block), lambda i: (0, jnp.minimum(i, steps - 1))),
        pl.BlockSpec((tokens, cols), lambda i: (0, 0)),
    ]
    args = [base, left, right]
    aliases = {}
    if previous is not None:
        in_specs.append(pl.BlockSpec(memory_space=pl.ANY))
        args.append(previous)
        aliases = {3: 0}
    return pl.pallas_call(
        kernel,
        grid=(steps + 1,),
        in_specs=in_specs,
        out_specs=[
            pl.BlockSpec((block, cols), lambda i: (start + jnp.maximum(i - 1, 0), 0)),
            pl.BlockSpec((8, cols), lambda i: (0, 0)),
        ],
        out_shape=[
            jax.ShapeDtypeStruct((rows, cols), jnp.float32),
            jax.ShapeDtypeStruct((8, cols), jnp.float32),
        ],
        scratch_shapes=[pltpu.VMEM((2, tokens, block), jnp.bfloat16)],
        input_output_aliases=aliases,
        compiler_params=pltpu.CompilerParams(vmem_limit_bytes=56 * 1024 * 1024),
        name="correlate",
    )(*args)


def swap(x, axis, k):
    if k == 0:
        return x
    return lax.ppermute(x, axis, [(i, i ^ k) for i in range(lax.axis_size(axis))])


def shards(view_a, view_b):
    tokens, width = view_a.shape
    n_row = lax.axis_size("row")
    n_col = lax.axis_size("col")
    row = lax.axis_index("row")
    col = lax.axis_index("col")
    count = tokens * n_row * n_col
    rows = width // n_row
    cols = width // n_col

    to_rows = [lax.dynamic_slice_in_dim(view_a, (row ^ k) * rows, rows, 1) for k in range(n_row)]
    to_cols = [lax.dynamic_slice_in_dim(view_b, (col ^ k) * cols, cols, 1) for k in range(n_col)]
    to_rows, to_cols = lax.optimization_barrier((to_rows, to_cols))
    right, left = [], []
    for k, x in enumerate(to_cols):
        right.append(swap(x, "col", k))
    for k, x in enumerate(to_rows):
        left.append(swap(x, "row", k))
    left = jnp.stack(left)
    right = jnp.stack(right)
    right = normalize([swap(right, "row", k) for k in range(n_row)], col, count)

    step = rows // CHUNKS
    gathered = [
        lax.all_gather(left[:, :, q * step:(q + 1) * step].reshape(n_row * tokens, step), "col", axis=0, tiled=True)
        for q in range(CHUNKS)
    ]
    correlation = None
    parts = []
    for q in range(CHUNKS):
        base = jnp.stack([row * rows + q * step, col * cols]).astype(jnp.int32)
        correlation, part = correlate(gathered[q], right, base, rows, q * step, correlation, count)
        parts.append(part)
    loss = jnp.sum(sum(parts).reshape(8, -1, 128), 1)
    loss = jnp.broadcast_to(jnp.sum(loss), (8, 128))
    for axis, size in (("col", n_col), ("row", n_row)):
        k = 1
        while k < size:
            loss = loss + swap(loss, axis, k)
            k *= 2
    return (correlation, loss[0, 0] / width)


def solution(mesh):
    return jax.shard_map(
        shards,
        mesh=mesh,
        in_specs=(P(("row", "col"), None), P(("row", "col"), None)),
        out_specs=(P("row", "col"), P()),
        check_vma=False,
    )
```
